128 devices in a mesh: gx: 4 (over z), gy: 4 (over y), gz: 8 (over x, core).
Axes of the slice: x: 4, y: 4, z: 4, core: 2. Of those that a mesh axis runs over, the one named last changes fastest.
Arguments:
- positions: float32 [3, 64, 64, 2048], P(None, 'gx', 'gy', 'gz'), may hold values from -6 to 6
- pair_node: int32 [4, 4, 8, 32, 256], P('gx', 'gy', 'gz'), may hold values from 0 to 255
- pair_line: int32 [4, 4, 8, 32], P('gx', 'gy', 'gz'), may hold values from 0 to 255
- pair_far: int32 [4, 4, 8, 32, 256], P('gx', 'gy', 'gz'), may hold values from 0 to 261, as said below
- far_line: int32 [4, 4, 8, 32], P('gx', 'gy', 'gz'), may hold values from 0 to 483, as said below
- pair_geom: float32 [4, 4, 8, 32, 4, 256], P('gx', 'gy', 'gz'), may hold values from -4 to 4
- live_blocks: int32 [4, 4, 8], P('gx', 'gy', 'gz'), may hold values from 8 to 32, as said below
Outputs:
- corrected: float32 [3, 64, 64, 2048], P(None, 'gx', 'gy', 'gz')
- sweep_history: float32 [2, 5], replicated
The draws below stay inside these ranges and needn't reach their ends.
Inputs may be any that keep to these rules, and one draw needn't show every extreme that they name: `pair_far`: together with far_line: at most one of the three coordinates of node b lies outside the owner block's own nodes; node b lies inside the whole grid; in slots below 16 node b is one of the owner block's own nodes. `far_line`: together with pair_far, as stated there. `live_blocks`: some owner block has all 32 slots live.
All inputs are finite; a program needn't handle non-finite values.
Results may differ from the reference program's by a relative error of at most 0.0001.
Values sent between devices are 32-bit elements; how exact they have to be, the bound alone decides.
A program may use at most 64 MiB of HBM per device.

```python
import jax
import jax.numpy as jnp
from jax import lax

CX = 16
CY = 16
CZ = 256
BLOCKS = 32
PAIRS_BLK = 256
RIM = 3
SWEEPS = 5
NX = 64
NY = 64
NZ = 2048
PAIRS_ALL = 1048576
N_GX = 4
N_GY = 4
N_GZ = 8


def far_layout(key):
    grid_x = NX // CX
    grid_y = NY // CY
    grid_z = NZ // CZ
    block_shape = (grid_x, grid_y, grid_z, BLOCKS)
    full_shape = (grid_x, grid_y, grid_z, BLOCKS, PAIRS_BLK)
    subkeys = jax.random.split(jax.random.fold_in(key, 7117), 8)
    line_x = jax.random.randint(subkeys[0], block_shape, RIM, CX + RIM)
    line_y = jax.random.randint(subkeys[1], block_shape, RIM, CY + RIM)
    coord_z = jax.random.randint(subkeys[2], full_shape, RIM, CZ + RIM)
    face_axis = jax.random.randint(subkeys[3], block_shape, 0, 3)
    high_block = jax.random.randint(subkeys[4], block_shape, 0, 2)
    layer_block = jax.random.randint(subkeys[5], block_shape, 0, RIM)
    high_pair = jax.random.randint(subkeys[6], full_shape, 0, 2)
    layer_pair = jax.random.randint(subkeys[7], full_shape, 0, RIM)
    rim_slot = lax.broadcasted_iota(jnp.int32, block_shape, 3) >= BLOCKS // 2

    def rim_coord(shape, axis_dim, extent, blocks_along, high_face, rim_layer):
        block_pos = lax.broadcasted_iota(jnp.int32, shape, axis_dim)
        low_side = jnp.where(block_pos == 0, RIM + rim_layer, rim_layer)
        high_side = jnp.where(block_pos == blocks_along - 1, extent + RIM - 1 - rim_layer, extent + RIM + rim_layer)
        return jnp.where(high_face == 1, high_side, low_side)
    line_x = jnp.where(rim_slot & (face_axis == 0), rim_coord(block_shape, 0, CX, grid_x, high_block, layer_block), line_x)
    line_y = jnp.where(rim_slot & (face_axis == 1), rim_coord(block_shape, 1, CY, grid_y, high_block, layer_block), line_y)
    z_face = (rim_slot & (face_axis == 2))[:, :, :, :, None]
    coord_z = jnp.where(z_face, rim_coord(full_shape, 2, CZ, grid_z, high_pair, layer_pair), coord_z)
    return ((line_x * (CY + 2 * RIM) + line_y).astype(jnp.int32), coord_z.astype(jnp.int32))


def draw_pair_far(key, part):
    return far_layout(key)[1]


def draw_far_line(key, part):
    return far_layout(key)[0]


def draw_live_blocks(key, part):
    grid_x = NX // CX
    grid_y = NY // CY
    grid_z = NZ // CZ
    full_shape = (grid_x, grid_y, grid_z)
    subkeys = jax.random.split(key, 3)
    base_count = jax.random.randint(subkeys[0], full_shape, BLOCKS // 4, BLOCKS // 2 + 1)
    heavy_dev = jax.random.randint(subkeys[1], full_shape, 0, 8) == 0
    chosen = jax.random.randint(subkeys[2], (), 0, grid_x * grid_y * grid_z)
    linear = (lax.broadcasted_iota(jnp.int32, full_shape, 0) * grid_y + lax.broadcasted_iota(jnp.int32, full_shape, 1)) * grid_z + lax.broadcasted_iota(jnp.int32, full_shape, 2)
    return jnp.where(heavy_dev | (linear == chosen), BLOCKS, base_count).astype(jnp.int32)


def set_ends(drawn, own_key, low, top_value):
    longest = drawn.shape.index(max(drawn.shape))
    spots = []
    for shift in (0, 1):
        where = [jax.random.randint(jax.random.fold_in(own_key, axis), (), 0, length) for axis, length in enumerate(drawn.shape)]
        where[longest] = (where[longest] + shift) % drawn.shape[longest]
        spots.append(tuple(where))
    return drawn.at[spots[0]].set(low).at[spots[1]].set(top_value)


def shard_levels(stream_key, dims, cuts, least, top_value):
    level = 1.0
    for dim, shards_of in cuts:
        steps = jax.random.uniform(jax.random.fold_in(jax.random.fold_in(stream_key, 6), dim), (shards_of,), jnp.float32, least / len(cuts), top_value / len(cuts))
        level = level * jnp.repeat(jnp.exp(steps), dims[dim] // shards_of).reshape((-1,) + (1,) * (len(dims) - 1 - dim))
    return level


def centred(own_key, shape, width, most, cuts=(), kind=jnp.bfloat16):
    gain = shard_levels(own_key, shape, cuts, -0.22, 0.18) if cuts else 1.0
    drawn = jax.random.normal(own_key, shape, jnp.float32) * width * gain
    return jnp.minimum(jnp.maximum(drawn, -most), most).astype(kind)


def setup_inputs(seed: int = 0) -> dict:
    seeds = jax.random.split(jax.random.key(seed), 8)
    return {
        "positions": centred(seeds[0], (3, NX, NY, NZ), 1.0, 6.0, ((1, 4), (2, 4), (3, 8)), jnp.float32),
        "pair_node": set_ends(jax.random.randint(seeds[1], (N_GX, N_GY, N_GZ, BLOCKS, PAIRS_BLK), 0, CZ), jax.random.fold_in(seeds[1], 1), 0, CZ - 1).astype(jnp.int32),
        "pair_line": set_ends(jax.random.randint(seeds[2], (N_GX, N_GY, N_GZ, BLOCKS), 0, CX * CY), jax.random.fold_in(seeds[2], 1), 0, (CX * CY) - 1).astype(jnp.int32),
        "pair_far": draw_pair_far(jax.random.fold_in(seeds[7], 71), 0),
        "far_line": draw_far_line(jax.random.fold_in(seeds[7], 71), 0),
        "pair_geom": centred(seeds[5], (N_GX, N_GY, N_GZ, BLOCKS, 4, PAIRS_BLK), 0.6, 4.0, ((0, 4), (1, 4), (2, 8)), jnp.float32),
        "live_blocks": draw_live_blocks(jax.random.fold_in(seeds[7], 71), 0),
    }


relax_factor = 0.9

def reference(positions, pair_node, pair_line, pair_far, far_line, pair_geom, live_blocks):
    full_shape = pair_node.shape
    block_x = lax.broadcasted_iota(jnp.int32, full_shape, 0)
    block_y = lax.broadcasted_iota(jnp.int32, full_shape, 1)
    block_z = lax.broadcasted_iota(jnp.int32, full_shape, 2)
    slot_index = lax.broadcasted_iota(jnp.int32, full_shape, 3)
    line_full = jnp.broadcast_to(pair_line[:, :, :, :, None], full_shape)
    node_x = block_x * CX + line_full // CY
    node_y = block_y * CY + line_full % CY
    node_z = block_z * CZ + pair_node
    own_flat = ((node_x * NY + node_y) * NZ + node_z).reshape(-1).astype(jnp.int32)
    ext_y = CY + 2 * RIM
    far_full = jnp.broadcast_to(far_line[:, :, :, :, None], full_shape)
    far_x = far_full // ext_y
    far_y = far_full % ext_y
    far_z = pair_far
    pad_y = NY + 2 * RIM
    pad_z = NZ + 2 * RIM
    far_flat = (((block_x * CX + far_x) * pad_y + block_y * CY + far_y) * pad_z + block_z * CZ + far_z).reshape(-1).astype(jnp.int32)
    live_mask = (slot_index < live_blocks[:, :, :, None, None]).reshape(-1)
    geometry = jnp.moveaxis(pair_geom, 4, 0).reshape(4, -1)
    node_count = NX * NY * NZ
    live_ones = jnp.where(live_mask, 1.0, 0.0).astype(jnp.float32)
    counts = jnp.zeros((node_count,), jnp.float32).at[own_flat].add(live_ones)
    current = positions.reshape(3, -1)
    energies = []
    residuals = []
    for sweep_idx in range(SWEEPS):
        padded = jnp.pad(current.reshape(3, NX, NY, NZ), ((0, 0), (RIM, RIM), (RIM, RIM), (RIM, RIM))).reshape(3, -1)
        differ = current[:, own_flat] - padded[:, far_flat]
        gap_value = lax.optimization_barrier(jnp.sum(geometry[0:3] * differ, axis=0)) - geometry[3]
        depth_value = jnp.where(live_mask, jnp.maximum(-gap_value, 0.0), 0.0)
        energy = jnp.sum(depth_value * depth_value)
        node_total = jnp.zeros((3, node_count), jnp.float32).at[:, own_flat].add(depth_value[None, :] * geometry[0:3])
        scale_factor = 1.0 / (1.0 + energy / PAIRS_ALL)
        correction = relax_factor * scale_factor * node_total / (1.0 + counts)
        current = current + correction
        residuals.append(jnp.sum(correction * correction))
        energies.append(energy)
    history = jnp.stack([jnp.sqrt(1.0 + jnp.stack(energies) / (PAIRS_BLK * BLOCKS)), jnp.sqrt(1.0 + jnp.stack(residuals) / (CX * CY * CZ))])
    return (current.reshape(3, NX, NY, NZ), history)
```

```python
import functools
import itertools

import jax
import jax.numpy as jnp
from jax import lax
from jax.experimental import pallas as pl
from jax.experimental.pallas import tpu as pltpu
from jax.sharding import PartitionSpec as P

RIM = 3
SWEEPS = 5
RELAX = 0.9
AXES = ("gx", "gy", "gz")
MESH = pl.DeviceIdType.MESH
f32 = jnp.float32
bf16 = jnp.bfloat16
i32 = jnp.int32
DIRS = [(a, s) for a in (1, 0, 2) for s in (1, -1)]


def scope(name):
    return jax.named_scope(name)


def split(x, parts):
    out = []
    for _ in range(parts - 1):
        hi = x.astype(bf16)
        out.append(hi)
        x = x - hi.astype(f32)
    out.append(x.astype(bf16))
    return out


def mm(a, b):
    return jnp.dot(a, b, preferred_element_type=f32)


def cat(parts):
    return jnp.concatenate(parts, axis=0)


def take_lanes(x, low, half):
    outs = []
    for h in range(0, low.shape[1], 128):
        idx = low[:, h : h + 128]
        got = jnp.take_along_axis(x[:, :128], idx, axis=1, mode="promise_in_bounds")
        for j in range(1, x.shape[1] // 128):
            more = jnp.take_along_axis(
                x[:, 128 * j : 128 * (j + 1)], idx, axis=1, mode="promise_in_bounds"
            )
            got = jnp.where(half[:, h : h + 128] == j, more, got)
        outs.append(got)
    return jnp.concatenate(outs, axis=1)


def kernel(
    sizes,
    blk,
    live_hbm,
    node_hbm,
    line_hbm,
    far_hbm,
    farline_hbm,
    geom_hbm,
    pos_hbm,
    out_ref,
    hist_ref,
    pos_v,
    node_v,
    far_v,
    geom_v,
    line_v,
    farline_v,
    live_v,
    rfar,
    rline,
    rgeom,
    ppart,
    hot,
    amat,
    geo,
    low_ref,
    half_ref,
    cinv,
    gap,
    wcat,
    acc,
    track,
    vsend,
    vrecv,
    dsend,
    drecv,
    erecv,
    rrecv,
    in_sem,
    qs_sem,
    qr_sem,
    vs_sem,
    vr_sem,
    ds_sem,
    dr_sem,
    es_sem,
    er_sem,
    rs_sem,
    rr_sem,
    plane_sem,
    all_sem,
):
    nx, ny, nz = sizes
    bx, by, bz = blk
    devices = nx * ny * nz
    blocks, pairs = gap.shape
    outer = blocks // 2
    lines = bx * by
    base = len(DIRS) * outer
    me = [lax.axis_index(a) for a in AXES]
    mine = (me[0] * ny + me[1]) * nz + me[2]

    def at_offset(off):
        return tuple(lax.rem(me[a] + off[a], sizes[a]) if off[a] else me[a] for a in range(3))

    def neighbour(axis, sign):
        off = [0, 0, 0]
        off[axis] = sign % sizes[axis]
        return at_offset(off)

    def exists(axis, sign):
        return (me[axis] + sign >= 0) & (me[axis] + sign < sizes[axis])

    def along(axis):
        return [tuple(o if a == axis else 0 for a in range(3)) for o in range(1, sizes[axis])]

    with scope("entry"):
        barrier = pltpu.get_barrier_semaphore()
        close = along(2) + along(1) + along(0)
        for off in close:
            pl.semaphore_signal(barrier, inc=1, device_id=at_offset(off), device_id_type=MESH)
        loads = [
            pltpu.make_async_copy(src, dst, in_sem.at[i])
            for i, (src, dst) in enumerate(
                [
                    (far_hbm.at[0, 0, 0], far_v),
                    (farline_hbm.at[0, 0], farline_v),
                    (geom_hbm.at[0, 0, 0], geom_v),
                    (pos_hbm, pos_v),
                    (node_hbm.at[0, 0, 0], node_v),
                    (line_hbm.at[0, 0], line_v),
                    (live_hbm.at[0], live_v),
                ]
            )
        ]
        for load in loads:
            load.start()
        loads[0].wait()
        loads[1].wait()
        pl.semaphore_wait(barrier, len(close))

    asks = [
        (far_v.at[pl.ds(outer, outer)], rfar),
        (farline_v, rline),
        (geom_v.at[pl.ds(outer, outer)], rgeom),
    ]

    def ask(i, d, axis, sign):
        return pltpu.make_async_remote_copy(
            src_ref=asks[i][0],
            dst_ref=asks[i][1].at[d],
            send_sem=qs_sem.at[i, d],
            recv_sem=qr_sem.at[i, d],
            device_id=neighbour(axis, sign),
            device_id_type=MESH,
        )

    with scope("ask"):
        for d, (axis, sign) in enumerate(DIRS):

            @pl.when(exists(axis, sign))
            def _():
                ask(1, d, axis, sign).start()
                ask(0, d, axis, sign).start()

        for off in along(1):
            pl.semaphore_signal(plane_sem, inc=1, device_id=at_offset(off), device_id_type=MESH)
        loads[2].wait()
        for d, (axis, sign) in enumerate(DIRS):

            @pl.when(exists(axis, sign))
            def _():
                ask(2, d, axis, sign).start()

            @pl.when(jnp.logical_not(exists(axis, -sign)))
            def _():
                rfar[d] = jnp.zeros((outer, pairs), i32)
                rline[d] = jnp.zeros((1, blocks), i32)
                rgeom[d] = jnp.zeros((outer, 4, pairs), f32)

            @pl.when(jnp.logical_not(exists(axis, sign)))
            def _():
                vrecv[d] = jnp.zeros((3, outer, pairs), f32)
                for t in range(SWEEPS - 1):
                    drecv[t, d] = jnp.zeros((outer, pairs), f32)

    with scope("parts"):
        loads[3].wait()
        for c in range(3):
            for i, part in enumerate(split(pos_v[c].reshape(lines, bz), 3)):
                ppart[c, i] = part

    with scope("hot"):
        for load in loads[4:]:
            load.wait()
        lane_node = lax.broadcasted_iota(i32, (pairs, bz), 1).astype(f32)
        node_t = jnp.transpose(node_v[...].astype(f32))
        for b in range(blocks):
            hot[pl.ds(b * pairs, pairs), :] = jnp.where(
                node_t[:, b : b + 1] == lane_node, 1.0, 0.0
            ).astype(bf16)

    row_line = line_v[...].astype(f32)
    two = jnp.concatenate([row_line, row_line], axis=1)
    lane_line = lax.broadcasted_iota(i32, (1, lines), 1).astype(f32)

    def column(row, first, n):
        r = lax.broadcasted_iota(i32, (n, blocks), 0)
        l = lax.broadcasted_iota(i32, (n, blocks), 1)
        return jnp.sum(jnp.where(l == r + first, row, 0.0), axis=1, keepdims=True)

    def located(code, zpos, shift):
        e = jnp.floor((code + 0.5) / (by + 2 * RIM))
        f = code - e * (by + 2 * RIM)
        e = e - (RIM + shift[0] * bx)
        f = f - (RIM + shift[1] * by)
        z = zpos - (RIM + shift[2] * bz)
        ok_line = (e >= 0) & (e < bx) & (f >= 0) & (f < by)
        ok = ok_line & (z >= 0) & (z < bz)
        return jnp.where(ok_line, e * by + f, -1.0), jnp.where(ok, z, 0.0), ok

    def place(row, line, node):
        n = line.shape[0]
        amat[pl.ds(row, n), :] = jnp.where(line == two, 1.0, 0.0).astype(bf16)
        idx = node.astype(i32)
        low = lax.bitwise_and(idx, 127)
        half = lax.shift_right_logical(idx, 7)
        low_ref[pl.ds(row, n), :] = low
        half_ref[pl.ds(row, n), :] = half
        own = jnp.where(line == lane_line, 1.0, 0.0).astype(bf16)
        out = []
        for c in range(3):
            vals = mm(own, ppart[c, 0]) + mm(own, ppart[c, 1]) + mm(own, ppart[c, 2])
            out.append(take_lanes(vals, low, half))
        return out

    with scope("known"):
        pl.semaphore_wait(plane_sem, ny - 1)
        for off in along(2):
            pl.semaphore_signal(all_sem, inc=1, device_id=at_offset(off), device_id_type=MESH)

    with scope("ask_wait"):
        for d, (axis, sign) in enumerate(DIRS):

            @pl.when(exists(axis, -sign))
            def _():
                ask(1, d, axis, sign).wait_recv()
                ask(0, d, axis, sign).wait_recv()

    def give(d, axis, sign):
        return pltpu.make_async_remote_copy(
            src_ref=vsend.at[d],
            dst_ref=vrecv.at[d],
            send_sem=vs_sem.at[d],
            recv_sem=vr_sem.at[d],
            device_id=neighbour(axis, -sign),
            device_id_type=MESH,
        )

    with scope("give"):
        asked_line, asked_node, asked_ok = [], [], []
        for d, (axis, sign) in enumerate(DIRS):
            shift = [0, 0, 0]
            shift[axis] = sign
            code = column(rline[d].astype(f32), outer, outer)
            line, z, ok = located(code, rfar[d].astype(f32), shift)
            asked_line.append(line)
            asked_node.append(z)
            asked_ok.append(jnp.where(ok, 1.0, 0.0))
        asked_ok = cat(asked_ok)
        vals = place(0, cat(asked_line), cat(asked_node))
        for c in range(3):
            got = vals[c] * asked_ok
            for d in range(len(DIRS)):
                vsend[d, c] = got[d * outer : (d + 1) * outer]
        for d, (axis, sign) in enumerate(DIRS):

            @pl.when(exists(axis, -sign))
            def _():
                give(d, axis, sign).start()

    with scope("counts"):
        live = jnp.broadcast_to(live_v[...], (blocks, pairs))
        live_rows = lax.broadcasted_iota(i32, (blocks, pairs), 0) < live

        def expand(stack, step):
            rows = stack.shape[0]
            which = lax.rem(lax.broadcasted_iota(i32, (rows, pairs), 0), step)
            return jnp.concatenate(
                [jnp.where(which == j, stack, 0.0).astype(bf16) for j in range(step)], axis=1
            )

        counts = []
        for g in range(blocks // 8):
            ones = jnp.where(live_rows[8 * g : 8 * g + 8], 1.0, 0.0)
            counts.append(mm(expand(ones, 8), hot[pl.ds(8 * g * pairs, 8 * pairs), :]))
        counts = cat(counts).astype(bf16)
        line_col = column(row_line, 0, blocks)
        same = line_col == row_line
        row_mod = lax.broadcasted_iota(i32, (blocks, blocks), 0)
        col_mod = lax.broadcasted_iota(i32, (blocks, blocks), 1)
        first_col = 1.0 - jnp.max(
            jnp.where(same & (col_mod < row_mod), 1.0, 0.0), axis=1, keepdims=True
        )
        cinv[...] = RELAX / (1.0 + mm(jnp.where(same, 1.0, 0.0).astype(bf16), counts))

    with scope("own"):
        code = column(farline_v[...].astype(f32), 0, blocks)
        line, z, ok = located(code, far_v[...].astype(f32), (0, 0, 0))
        here = jnp.where(ok, 1.0, 0.0)
        vals = place(base, cat([line_col, line]), cat([node_v[...].astype(f32), z]))
        start = -geom_v[:, 3, :]
        for c in range(3):
            g = geom_v[:, c, :]
            away = -(g * here)
            geo[c, pl.ds(base, blocks), :] = g
            geo[c, pl.ds(base + blocks, blocks), :] = away
            start += g * vals[c][:blocks] + away * vals[c][blocks:]
        gap[...] = start
        acc[...] = jnp.zeros_like(acc)
        track[...] = jnp.zeros_like(track)
        rrecv[mine] = jnp.zeros((1, 128), f32)

    with scope("geo"):
        for d, (axis, sign) in enumerate(DIRS):

            @pl.when(exists(axis, -sign))
            def _():
                ask(2, d, axis, sign).wait_recv()

        for d in range(len(DIRS)):
            for c in range(3):
                rows = slice(d * outer, (d + 1) * outer)
                geo[c, rows, :] = -(rgeom[d, :, c, :] * asked_ok[rows])

    with scope("give_wait"):
        pl.semaphore_wait(all_sem, nz - 1)
        for d, (axis, sign) in enumerate(DIRS):

            @pl.when(exists(axis, sign))
            def _():
                give(d, axis, sign).wait_recv()

        more = jnp.zeros((outer, pairs), f32)
        for c in range(3):
            far = vrecv[0, c]
            for d in range(1, len(DIRS)):
                far = far + vrecv[d, c]
            more = more + geom_v[outer:, c, :] * far
        gap[pl.ds(outer, outer), :] = gap[pl.ds(outer, outer), :] - more

    def answer(t, d, axis, sign):
        return pltpu.make_async_remote_copy(
            src_ref=dsend.at[t, d],
            dst_ref=drecv.at[t, d],
            send_sem=ds_sem.at[t, d],
            recv_sem=dr_sem.at[t, d],
            device_id=neighbour(axis, -sign),
            device_id_type=MESH,
        )

    def hops(off):
        x, core = off[2] // 2, off[2] % 2
        far = [min(o, s - o) for o, s in ((off[0], nx), (off[1], ny), (x, nz // 2))]
        return sum(far) + 0.3 * core

    everyone = sorted(
        (o for o in itertools.product(range(nx), range(ny), range(nz)) if any(o)),
        key=hops,
        reverse=True,
    )

    def to_all(ref, send_sem, recv_sem):
        for off in everyone:
            pltpu.make_async_remote_copy(
                src_ref=ref,
                dst_ref=ref,
                send_sem=send_sem,
                recv_sem=recv_sem,
                device_id=at_offset(off),
                device_id_type=MESH,
            ).start()

    def lanes_sum(x):
        x = jnp.sum(x, axis=0, keepdims=True)
        out = x[:, :128]
        for j in range(1, x.shape[1] // 128):
            out = out + x[:, 128 * j : 128 * (j + 1)]
        return out

    lane = lax.broadcasted_iota(i32, (1, 128), 1)

    def dots(row, n, moved):
        low = low_ref[row : row + n, :]
        half = half_ref[row : row + n, :]
        total = geo[0, row : row + n] * take_lanes(moved[:, :bz], low, half)
        for c in range(1, 3):
            total += geo[c, row : row + n] * take_lanes(
                moved[:, c * bz : (c + 1) * bz], low, half
            )
        return total

    def sweep(t, last):
        with scope("energy"):
            depth = jnp.where(live_rows, jnp.maximum(-gap[...], 0.0), 0.0)
            squares = lanes_sum(depth * depth)
            if not last:
                erecv[t, mine] = squares
                to_all(erecv.at[t, mine], es_sem.at[t], er_sem.at[t])
        with scope("scatter"):
            for g in range(blocks // 8):
                lo, hi = 8 * g, 8 * g + 8
                terms = cat(
                    [depth[lo:hi] * geo[c, base + lo : base + hi] for c in range(3)]
                )
                top = terms.astype(bf16).astype(f32)
                sums = mm(
                    expand(cat([top, terms - top]), 8), hot[pl.ds(lo * pairs, 8 * pairs), :]
                )
                sums = sums[:24] + sums[24:]
                for c in range(3):
                    wcat[lo:hi, c * bz : (c + 1) * bz] = (
                        sums[8 * c : 8 * c + 8] * cinv[lo:hi, :]
                    )
            parts = cat(split(wcat[...], 2))
        if not last:
            with scope("respond"):
                total = dots(0, base, mm(amat[0:base, :], parts))
                for d in range(len(DIRS)):
                    dsend[t, d] = total[d * outer : (d + 1) * outer]
                for d, (axis, sign) in enumerate(DIRS):

                    @pl.when(exists(axis, -sign))
                    def _():
                        answer(t, d, axis, sign).start()

        with scope("resid"):
            moved = mm(amat[base : base + (blocks if last else 2 * blocks), :], parts)
            near = moved[:blocks]
            resid = jnp.sum(lanes_sum(near * near * first_col), axis=1, keepdims=True)
            rrecv[mine] = jnp.where(lane == t, resid, rrecv[mine])
        if last:
            energy = jnp.sum(squares, axis=1, keepdims=True)
            rrecv[mine] = jnp.where(lane == SWEEPS, energy, rrecv[mine])
            to_all(rrecv.at[mine], rs_sem, rr_sem)
            with scope("join"):
                row = lax.broadcasted_iota(i32, (lines, 2 * blocks), 0).astype(f32)
                spread = jnp.where(row == two, 1.0, 0.0).astype(bf16)
                before = mm(spread, cat(split(acc[...], 2)))
                ahead = mm(spread, parts)
                for c in range(3):
                    pos_v[c] = pos_v[c] + before[:, c * bz : (c + 1) * bz].reshape(bx, by, bz)
                    out_ref[c] = ahead[:, c * bz : (c + 1) * bz].reshape(bx, by, bz)
            with scope("last_wait"):
                others = rrecv.at[pl.ds(0, devices - 1)]
                pltpu.make_async_copy(others, others, rr_sem).wait()
                energy = jnp.sum(rrecv[...], axis=0)[:, SWEEPS : SWEEPS + 1]
        else:
            with scope("step"):
                step = dots(base, 2 * blocks, moved)
                step = step[:blocks] + step[blocks:]
            with scope("energy_wait"):
                others = erecv.at[t, pl.ds(0, devices - 1)]
                pltpu.make_async_copy(others, others, er_sem.at[t]).wait()
                energy = jnp.sum(jnp.sum(erecv[t], axis=0), axis=1, keepdims=True)
        scale = 1.0 / (1.0 + energy / (blocks * pairs * devices))
        track[0:1, :] = jnp.where(lane == t, energy, track[0:1, :])
        track[1:2, :] = jnp.where(lane == t, scale, track[1:2, :])
        if last:
            for c in range(3):
                out_ref[c] = pos_v[c] + jnp.broadcast_to(scale[:, None], (1, 1, 1)) * out_ref[c]
            return
        with scope("answer_wait"):
            for d, (axis, sign) in enumerate(DIRS):

                @pl.when(exists(axis, sign))
                def _():
                    answer(t, d, axis, sign).wait_recv()

        more = drecv[t, 0]
        for d in range(1, len(DIRS)):
            more = more + drecv[t, d]
        acc[...] = acc[...] + scale * wcat[...]
        gap[0:outer, :] = gap[0:outer, :] + scale * step[:outer]
        gap[pl.ds(outer, outer), :] = gap[pl.ds(outer, outer), :] + scale * (step[outer:] + more)

    def body(t, carry):
        sweep(t, False)
        return carry

    lax.fori_loop(0, SWEEPS - 1, body, 0)
    sweep(SWEEPS - 1, True)

    with scope("end"):
        for d, (axis, sign) in enumerate(DIRS):

            @pl.when(exists(axis, sign))
            def _():
                for i in range(3):
                    ask(i, d, axis, sign).wait_send()

            @pl.when(exists(axis, -sign))
            def _():
                give(d, axis, sign).wait_send()
                for t in range(SWEEPS - 1):
                    answer(t, d, axis, sign).wait_send()

        for t in range(SWEEPS - 1):
            ref = erecv.at[t, pl.ds(0, devices - 1)]
            pltpu.make_async_copy(ref, ref, es_sem.at[t]).wait()
        others = rrecv.at[pl.ds(0, devices - 1)]
        pltpu.make_async_copy(others, others, rs_sem).wait()
        energy, scale = track[0:1, :], track[1:2, :]
        resid = jnp.sum(rrecv[...], axis=0)
        n = hist_ref.shape[1]
        hist_ref[0:1, :] = jnp.sqrt(1.0 + energy / (blocks * pairs))[:, :n]
        hist_ref[1:2, :] = jnp.sqrt(1.0 + scale * scale * resid / (bx * by * bz))[:, :n]


def local(sizes, positions, pair_node, pair_line, pair_far, far_line, pair_geom, live_blocks):
    blocks, pairs = pair_node.shape[3:]
    blk = positions.shape[1:]
    bx, by, bz = blk
    devices = sizes[0] * sizes[1] * sizes[2]
    outer = blocks // 2
    ndir = len(DIRS)
    rows = 2 * blocks + ndir * outer
    dma = pltpu.SemaphoreType.DMA
    vmem = pl.BlockSpec(memory_space=pltpu.VMEM)
    return pl.pallas_call(
        functools.partial(kernel, sizes, blk),
        out_shape=(
            jax.ShapeDtypeStruct(positions.shape, f32),
            jax.ShapeDtypeStruct((2, SWEEPS), f32),
        ),
        in_specs=[pl.BlockSpec(memory_space=pl.ANY)] * 7,
        out_specs=(vmem, vmem),
        scratch_shapes=[
            pltpu.VMEM(positions.shape, f32),
            pltpu.VMEM((blocks, pairs), i32),
            pltpu.VMEM((blocks, pairs), i32),
            pltpu.VMEM((blocks, 4, pairs), f32),
            pltpu.VMEM((1, blocks), i32),
            pltpu.VMEM((1, blocks), i32),
            pltpu.VMEM((1, 1), i32),
            pltpu.VMEM((ndir, outer, pairs), i32),
            pltpu.VMEM((ndir, 1, blocks), i32),
            pltpu.VMEM((ndir, outer, 4, pairs), f32),
            pltpu.VMEM((3, 3, bx * by, bz), bf16),
            pltpu.VMEM((blocks * pairs, bz), bf16),
            pltpu.VMEM((rows, 2 * blocks), bf16),
            pltpu.VMEM((3, rows, pairs), f32),
            pltpu.VMEM((rows, pairs), i32),
            pltpu.VMEM((rows, pairs), i32),
            pltpu.VMEM((blocks, bz), f32),
            pltpu.VMEM((blocks, pairs), f32),
            pltpu.VMEM((blocks, 3 * bz), f32),
            pltpu.VMEM((blocks, 3 * bz), f32),
            pltpu.VMEM((8, 128), f32),
            pltpu.VMEM((ndir, 3, outer, pairs), f32),
            pltpu.VMEM((ndir, 3, outer, pairs), f32),
            pltpu.VMEM((SWEEPS - 1, ndir, outer, pairs), f32),
            pltpu.VMEM((SWEEPS - 1, ndir, outer, pairs), f32),
            pltpu.VMEM((SWEEPS - 1, devices, 1, 128), f32),
            pltpu.VMEM((devices, 1, 128), f32),
            dma((7,)),
            dma((3, ndir)),
            dma((3, ndir)),
            dma((ndir,)),
            dma((ndir,)),
            dma((SWEEPS - 1, ndir)),
            dma((SWEEPS - 1, ndir)),
            dma((SWEEPS - 1,)),
            dma((SWEEPS - 1,)),
            dma,
            dma,
            pltpu.SemaphoreType.REGULAR,
            pltpu.SemaphoreType.REGULAR,
        ],
        compiler_params=pltpu.CompilerParams(collective_id=0, has_side_effects=True),
    )(live_blocks, pair_node, pair_line, pair_far, far_line, pair_geom, positions)


def solution(mesh):
    sizes = tuple(mesh.shape[a] for a in AXES)
    return jax.shard_map(
        functools.partial(local, sizes),
        mesh=mesh,
        in_specs=(
            P(None, "gx", "gy", "gz"),
            P("gx", "gy", "gz", None, None),
            P("gx", "gy", "gz", None),
            P("gx", "gy", "gz", None, None),
            P("gx", "gy", "gz", None),
            P("gx", "gy", "gz", None, None, None),
            P("gx", "gy", "gz"),
        ),
        out_specs=(P(None, "gx", "gy", "gz"), P()),
        check_vma=False,
    )
```

```python
import functools
import itertools

import jax
import jax.numpy as jnp
from jax import lax
from jax.experimental import pallas as pl
from jax.experimental.pallas import tpu as pltpu
from jax.sharding import PartitionSpec as P

RIM = 3
SWEEPS = 5
RELAX = 0.9
AXES = ("gx", "gy", "gz")
MESH = pl.DeviceIdType.MESH
f32 = jnp.float32
bf16 = jnp.bfloat16
i32 = jnp.int32
DIRS = [(a, s) for a in (1, 0, 2) for s in (1, -1)]


def scope(name):
    return jax.named_scope(name)


def split(x, parts):
    out = []
    for _ in range(parts - 1):
        hi = x.astype(bf16)
        out.append(hi)
        x = x - hi.astype(f32)
    out.append(x.astype(bf16))
    return out


def mm(a, b):
    return jnp.dot(a, b, preferred_element_type=f32)


def cat(parts):
    return jnp.concatenate(parts, axis=0)


def take_lanes(x, low, half):
    outs = []
    for h in range(0, low.shape[1], 128):
        idx = low[:, h : h + 128]
        got = jnp.take_along_axis(x[:, :128], idx, axis=1, mode="promise_in_bounds")
        for j in range(1, x.shape[1] // 128):
            more = jnp.take_along_axis(
                x[:, 128 * j : 128 * (j + 1)], idx, axis=1, mode="promise_in_bounds"
            )
            got = jnp.where(half[:, h : h + 128] == j, more, got)
        outs.append(got)
    return jnp.concatenate(outs, axis=1)


def kernel(
    sizes,
    blk,
    live_hbm,
    node_hbm,
    line_hbm,
    far_hbm,
    farline_hbm,
    geom_hbm,
    pos_hbm,
    out_ref,
    hist_ref,
    pos_v,
    node_v,
    far_v,
    geom_v,
    line_v,
    farline_v,
    live_v,
    rfar,
    rline,
    rgeom,
    ppart,
    hot,
    amat,
    geo,
    low_ref,
    half_ref,
    cinv,
    gap,
    depth_ref,
    delta,
    wcat,
    acc,
    track,
    vsend,
    vrecv,
    dsend,
    drecv,
    erecv,
    in_sem,
    qs_sem,
    qr_sem,
    as_sem,
    vr_sem,
    dr_sem,
    es_sem,
    er_sem,
    plane_sem,
    all_sem,
):
    nx, ny, nz = sizes
    bx, by, bz = blk
    devices = nx * ny * nz
    blocks, pairs = gap.shape
    outer = blocks // 2
    lines = bx * by
    base = len(DIRS) * outer
    me = [lax.axis_index(a) for a in AXES]
    mine = (me[0] * ny + me[1]) * nz + me[2]

    def at_offset(off):
        return tuple(lax.rem(me[a] + off[a], sizes[a]) if off[a] else me[a] for a in range(3))

    def neighbour(axis, sign):
        off = [0, 0, 0]
        off[axis] = sign % sizes[axis]
        return at_offset(off)

    def exists(axis, sign):
        return (me[axis] + sign >= 0) & (me[axis] + sign < sizes[axis])

    def along(axis):
        return [tuple(o if a == axis else 0 for a in range(3)) for o in range(1, sizes[axis])]

    with scope("entry"):
        barrier = pltpu.get_barrier_semaphore()
        close = along(2) + along(1) + along(0)
        for off in close:
            pl.semaphore_signal(barrier, inc=1, device_id=at_offset(off), device_id_type=MESH)
        loads = [
            pltpu.make_async_copy(src, dst, in_sem.at[i])
            for i, (src, dst) in enumerate(
                [
                    (far_hbm.at[0, 0, 0], far_v),
                    (farline_hbm.at[0, 0], farline_v),
                    (geom_hbm.at[0, 0, 0], geom_v),
                    (pos_hbm, pos_v),
                    (node_hbm.at[0, 0, 0], node_v),
                    (line_hbm.at[0, 0], line_v),
                    (live_hbm.at[0], live_v),
                ]
            )
        ]
        for load in loads:
            load.start()
        loads[0].wait()
        loads[1].wait()
        pl.semaphore_wait(barrier, len(close))

    asks = [
        (far_v.at[pl.ds(outer, outer)], rfar),
        (farline_v, rline),
        (geom_v.at[pl.ds(outer, outer)], rgeom),
    ]

    def ask(i, d, axis, sign):
        return pltpu.make_async_remote_copy(
            src_ref=asks[i][0],
            dst_ref=asks[i][1].at[d],
            send_sem=qs_sem.at[i % 2, d],
            recv_sem=qr_sem.at[i, d],
            device_id=neighbour(axis, sign),
            device_id_type=MESH,
        )

    with scope("ask"):
        for d, (axis, sign) in enumerate(DIRS):

            @pl.when(exists(axis, sign))
            def _():
                ask(1, d, axis, sign).start()
                ask(0, d, axis, sign).start()

        for off in along(1):
            pl.semaphore_signal(plane_sem, inc=1, device_id=at_offset(off), device_id_type=MESH)
        loads[2].wait()
        for d, (axis, sign) in enumerate(DIRS):

            @pl.when(exists(axis, sign))
            def _():
                ask(2, d, axis, sign).start()

            @pl.when(jnp.logical_not(exists(axis, -sign)))
            def _():
                rfar[d] = jnp.zeros((outer, pairs), i32)
                rline[d] = jnp.zeros((1, blocks), i32)
                rgeom[d] = jnp.zeros((outer, 4, pairs), f32)

            @pl.when(jnp.logical_not(exists(axis, sign)))
            def _():
                vrecv[d] = jnp.zeros((3, outer, pairs), f32)
                for t in range(SWEEPS - 1):
                    drecv[t, d] = jnp.zeros((outer, pairs), f32)

    with scope("parts"):
        loads[3].wait()
        for c in range(3):
            for i, part in enumerate(split(pos_v[c].reshape(lines, bz), 3)):
                ppart[c, i] = part

    with scope("hot"):
        for load in loads[4:]:
            load.wait()
        lane_node = lax.broadcasted_iota(i32, (pairs, bz), 1).astype(f32)
        node_t = jnp.transpose(node_v[...].astype(f32))
        for b in range(blocks):
            hot[pl.ds(b * pairs, pairs), :] = jnp.where(
                node_t[:, b : b + 1] == lane_node, 1.0, 0.0
            ).astype(bf16)

    row_line = line_v[...].astype(f32)
    two = jnp.concatenate([row_line, row_line], axis=1)
    lane_line = lax.broadcasted_iota(i32, (1, lines), 1).astype(f32)

    def column(row, first, n):
        r = lax.broadcasted_iota(i32, (n, blocks), 0)
        l = lax.broadcasted_iota(i32, (n, blocks), 1)
        return jnp.sum(jnp.where(l == r + first, row, 0.0), axis=1, keepdims=True)

    def located(code, zpos, shift):
        e = jnp.floor((code + 0.5) / (by + 2 * RIM))
        f = code - e * (by + 2 * RIM)
        e = e - (RIM + shift[0] * bx)
        f = f - (RIM + shift[1] * by)
        z = zpos - (RIM + shift[2] * bz)
        ok_line = (e >= 0) & (e < bx) & (f >= 0) & (f < by)
        ok = ok_line & (z >= 0) & (z < bz)
        return jnp.where(ok_line, e * by + f, -1.0), jnp.where(ok, z, 0.0), ok

    def place(row, line, node):
        n = line.shape[0]
        idx = node.astype(i32)
        low = lax.bitwise_and(idx, 127)
        half = lax.shift_right_logical(idx, 7)
        own = jnp.where(line == lane_line, 1.0, 0.0).astype(bf16)

        def value(c):
            vals = mm(own, ppart[c, 0]) + mm(own, ppart[c, 1]) + mm(own, ppart[c, 2])
            return take_lanes(vals, low, half)

        def keep():
            amat[pl.ds(row, n), :] = jnp.where(line == two, 1.0, 0.0).astype(bf16)
            low_ref[pl.ds(row, n), :] = low
            half_ref[pl.ds(row, n), :] = half

        return value, keep

    with scope("known"):
        pl.semaphore_wait(plane_sem, ny - 1)
        for off in along(2):
            pl.semaphore_signal(all_sem, inc=1, device_id=at_offset(off), device_id_type=MESH)

    with scope("ask_wait"):
        for d, (axis, sign) in enumerate(DIRS):

            @pl.when(exists(axis, -sign))
            def _():
                ask(1, d, axis, sign).wait_recv()
                ask(0, d, axis, sign).wait_recv()

    def give(c, d, axis, sign):
        return pltpu.make_async_remote_copy(
            src_ref=vsend.at[d, c],
            dst_ref=vrecv.at[d, c],
            send_sem=as_sem.at[d],
            recv_sem=vr_sem.at[d],
            device_id=neighbour(axis, -sign),
            device_id_type=MESH,
        )

    with scope("give"):
        asked_line, asked_node, asked_ok = [], [], []
        for d, (axis, sign) in enumerate(DIRS):
            shift = [0, 0, 0]
            shift[axis] = sign
            code = column(rline[d].astype(f32), outer, outer)
            line, z, ok = located(code, rfar[d].astype(f32), shift)
            asked_line.append(line)
            asked_node.append(z)
            asked_ok.append(jnp.where(ok, 1.0, 0.0))
        asked_ok = cat(asked_ok)
        value, keep = place(0, cat(asked_line), cat(asked_node))
        for c in range(3):
            got = value(c) * asked_ok
            for d in range(len(DIRS)):
                vsend[d, c] = got[d * outer : (d + 1) * outer]
            for d, (axis, sign) in enumerate(DIRS):

                @pl.when(exists(axis, -sign))
                def _():
                    give(c, d, axis, sign).start()

        keep()

    with scope("counts"):
        live = jnp.broadcast_to(live_v[...], (blocks, pairs))
        live_rows = lax.broadcasted_iota(i32, (blocks, pairs), 0) < live

        def expand(stack, step):
            rows = stack.shape[0]
            which = lax.rem(lax.broadcasted_iota(i32, (rows, pairs), 0), step)
            return jnp.concatenate(
                [jnp.where(which == j, stack, 0.0).astype(bf16) for j in range(step)], axis=1
            )

        counts = []
        for g in range(blocks // 8):
            ones = jnp.where(live_rows[8 * g : 8 * g + 8], 1.0, 0.0)
            counts.append(mm(expand(ones, 8), hot[pl.ds(8 * g * pairs, 8 * pairs), :]))
        counts = cat(counts).astype(bf16)
        line_col = column(row_line, 0, blocks)
        same = line_col == row_line
        row_mod = lax.broadcasted_iota(i32, (blocks, blocks), 0)
        col_mod = lax.broadcasted_iota(i32, (blocks, blocks), 1)
        first_col = 1.0 - jnp.max(
            jnp.where(same & (col_mod < row_mod), 1.0, 0.0), axis=1, keepdims=True
        )
        cinv[...] = RELAX / (1.0 + mm(jnp.where(same, 1.0, 0.0).astype(bf16), counts))

    with scope("own"):
        code = column(farline_v[...].astype(f32), 0, blocks)
        line, z, ok = located(code, far_v[...].astype(f32), (0, 0, 0))
        here = jnp.where(ok, 1.0, 0.0)
        value, keep = place(base, cat([line_col, line]), cat([node_v[...].astype(f32), z]))
        start = -geom_v[:, 3, :]
        for c in range(3):
            g = geom_v[:, c, :]
            away = -(g * here)
            geo[c, pl.ds(base, blocks), :] = g
            geo[c, pl.ds(base + blocks, blocks), :] = away
            vals = value(c)
            start += g * vals[:blocks] + away * vals[blocks:]
        keep()
        gap[...] = start
        acc[...] = jnp.zeros_like(acc)
        wcat[...] = jnp.zeros_like(wcat)
        track[...] = jnp.zeros_like(track)

    with scope("geo"):
        for d, (axis, sign) in enumerate(DIRS):

            @pl.when(exists(axis, -sign))
            def _():
                ask(2, d, axis, sign).wait_recv()

        for d in range(len(DIRS)):
            for c in range(3):
                rows = slice(d * outer, (d + 1) * outer)
                geo[c, rows, :] = -(rgeom[d, :, c, :] * asked_ok[rows])

    with scope("give_wait"):
        pl.semaphore_wait(all_sem, nz - 1)
        for d, (axis, sign) in enumerate(DIRS):

            @pl.when(exists(axis, sign))
            def _():
                pltpu.make_async_copy(vrecv.at[d], vrecv.at[d], vr_sem.at[d]).wait()

        more = jnp.zeros((outer, pairs), f32)
        for c in range(3):
            far = vrecv[0, c]
            for d in range(1, len(DIRS)):
                far = far + vrecv[d, c]
            more = more + geom_v[outer:, c, :] * far
        gap[pl.ds(outer, outer), :] = gap[pl.ds(outer, outer), :] - more

    def answer(t, d, axis, sign):
        return pltpu.make_async_remote_copy(
            src_ref=dsend.at[t, d],
            dst_ref=drecv.at[t, d],
            send_sem=as_sem.at[d],
            recv_sem=dr_sem.at[lax.rem(t, 2), d],
            device_id=neighbour(axis, -sign),
            device_id_type=MESH,
        )

    def hops(off):
        x, core = off[2] // 2, off[2] % 2
        far = [min(o, s - o) for o, s in ((off[0], nx), (off[1], ny), (x, nz // 2))]
        return sum(far) + 0.3 * core

    everyone = sorted(
        (o for o in itertools.product(range(nx), range(ny), range(nz)) if any(o)),
        key=hops,
        reverse=True,
    )

    def to_all(t):
        ref = erecv.at[t, mine]
        for off in everyone:
            pltpu.make_async_remote_copy(
                src_ref=ref,
                dst_ref=ref,
                send_sem=es_sem,
                recv_sem=er_sem.at[lax.rem(t, 2)],
                device_id=at_offset(off),
                device_id_type=MESH,
            ).start()

    def from_all(t):
        others = erecv.at[t, pl.ds(0, devices - 1)]
        pltpu.make_async_copy(others, others, er_sem.at[lax.rem(t, 2)]).wait()
        rows = [erecv[t, i] for i in range(devices)]
        while len(rows) > 1:
            rows = [a + b for a, b in zip(rows[::2], rows[1::2])] + rows[len(rows) & ~1 :]
        return rows[0]

    def lanes_sum(x):
        x = jnp.sum(x, axis=0, keepdims=True)
        out = x[:, :128]
        for j in range(1, x.shape[1] // 128):
            out = out + x[:, 128 * j : 128 * (j + 1)]
        return out

    lane = lax.broadcasted_iota(i32, (1, 128), 1)

    def dots(row, n, moved):
        low = low_ref[row : row + n, :]
        half = half_ref[row : row + n, :]
        total = geo[0, row : row + n] * take_lanes(moved[:, :bz], low, half)
        for c in range(1, 3):
            total += geo[c, row : row + n] * take_lanes(
                moved[:, c * bz : (c + 1) * bz], low, half
            )
        return total

    def depths():
        depth = jnp.where(live_rows, jnp.maximum(-gap[...], 0.0), 0.0)
        depth_ref[...] = depth
        return lanes_sum(depth * depth)

    def scatter():
        for g in range(blocks // 8):
            lo, hi = 8 * g, 8 * g + 8
            depth = depth_ref[lo:hi, :]
            terms = cat([depth * geo[c, base + lo : base + hi] for c in range(3)])
            top = terms.astype(bf16).astype(f32)
            sums = mm(expand(cat([top, terms - top]), 8), hot[pl.ds(lo * pairs, 8 * pairs), :])
            sums = sums[:24] + sums[24:]
            for c in range(3):
                wcat[lo:hi, c * bz : (c + 1) * bz] = sums[8 * c : 8 * c + 8] * cinv[lo:hi, :]
        return cat(split(wcat[...], 2))

    def residual(near):
        return jnp.sum(lanes_sum(near * near * first_col), axis=1, keepdims=True)

    def note(t, energy, scale):
        track[0:1, :] = jnp.where(lane == t, energy, track[0:1, :])
        track[1:2, :] = jnp.where(lane == t, scale, track[1:2, :])
        acc[...] = acc[...] + scale * wcat[...]

    def ratio(energy):
        return 1.0 / (1.0 + energy / (blocks * pairs * devices))

    def sweep(t, energy, last):
        with scope("note"):
            note(t - 1, energy, ratio(energy))
        with scope("scatter"):
            parts = scatter()
        with scope("respond"):
            total = dots(0, base, mm(amat[0:base, :], parts))
            for d in range(len(DIRS)):
                dsend[t, d] = total[d * outer : (d + 1) * outer]
            for d, (axis, sign) in enumerate(DIRS):

                @pl.when(exists(axis, -sign))
                def _():
                    answer(t, d, axis, sign).start()

        with scope("step"):
            moved = mm(amat[base : base + 2 * blocks, :], parts)
            resid = residual(moved[:blocks])
            track[2:3, :] = jnp.where(lane == t, resid, track[2:3, :])
            step = dots(base, 2 * blocks, moved)
            delta[...] = step[:blocks] + step[blocks:]
        with scope("answer_wait"):
            for d, (axis, sign) in enumerate(DIRS):

                @pl.when(exists(axis, sign))
                def _():
                    answer(t, d, axis, sign).wait_recv()

            more = drecv[t, 0]
            for d in range(1, len(DIRS)):
                more = more + drecv[t, d]
            delta[pl.ds(outer, outer), :] = delta[pl.ds(outer, outer), :] + more
        with scope("energy_wait"):
            energy = jnp.sum(from_all(t), axis=1, keepdims=True)
        with scope("energy"):
            gap[...] = gap[...] + ratio(energy) * delta[...]
            squares = depths()
            if last:
                return energy, squares
            erecv[t + 1, mine] = squares
            to_all(t + 1)
        return energy

    with scope("energy"):
        erecv[0, mine] = depths()
        to_all(0)

    zero = jnp.zeros((1, 1), f32)
    energy = lax.fori_loop(0, SWEEPS - 2, lambda t, energy: sweep(t, energy, False), zero)
    energy, squares = sweep(SWEEPS - 2, energy, True)
    end = SWEEPS - 1
    with scope("scatter"):
        note(end - 1, energy, ratio(energy))
        parts = scatter()
    with scope("resid"):
        resid = residual(mm(amat[base : base + blocks, :], parts))
        energy = jnp.sum(squares, axis=1, keepdims=True)
        row = jnp.where(lane == end, resid, track[2:3, :])
        erecv[end, mine] = jnp.where(lane == SWEEPS, energy, row)
        to_all(end)
    with scope("join"):
        row = lax.broadcasted_iota(i32, (lines, 2 * blocks), 0).astype(f32)
        spread = jnp.where(row == two, 1.0, 0.0).astype(bf16)
        before = mm(spread, cat(split(acc[...], 2)))
        ahead = mm(spread, parts)
        for c in range(3):
            pos_v[c] = pos_v[c] + before[:, c * bz : (c + 1) * bz].reshape(bx, by, bz)
            out_ref[c] = ahead[:, c * bz : (c + 1) * bz].reshape(bx, by, bz)
        for d, (axis, sign) in enumerate(DIRS):

            @pl.when(exists(axis, sign))
            def _():
                sent = geo.at[0, pl.ds(0, 5 * outer)]
                pltpu.make_async_copy(sent, sent, qs_sem.at[0, d]).wait()
                ask(1, d, axis, sign).wait_send()

            @pl.when(exists(axis, -sign))
            def _():
                sent = geo.at[0, pl.ds(0, (SWEEPS + 2) * outer)]
                pltpu.make_async_copy(sent, sent, as_sem.at[d]).wait()

    with scope("last_wait"):
        sums = from_all(end)
    with scope("end"):
        energy = sums[:, SWEEPS : SWEEPS + 1]
        scale = ratio(energy)
        for c in range(3):
            out_ref[c] = pos_v[c] + jnp.broadcast_to(scale[:, None], (1, 1, 1)) * out_ref[c]
        n = hist_ref.shape[1]
        energies = jnp.where(lane == end, energy, track[0:1, :])
        scales = jnp.where(lane == end, scale, track[1:2, :])
        hist_ref[0:1, :] = jnp.sqrt(1.0 + energies / (blocks * pairs))[:, :n]
        hist_ref[1:2, :] = jnp.sqrt(1.0 + scales * scales * sums / (bx * by * bz))[:, :n]
        sent = erecv.at[pl.ds(0, SWEEPS), pl.ds(0, devices - 1)]
        pltpu.make_async_copy(sent, sent, es_sem).wait()


def finish(moved, hist, out_hbm, hist_hbm, sem):
    copies = [
        pltpu.make_async_copy(moved, out_hbm, sem.at[0]),
        pltpu.make_async_copy(hist, hist_hbm, sem.at[1]),
    ]
    for copy in copies:
        copy.start()
    for copy in copies:
        copy.wait()


def local(sizes, positions, pair_node, pair_line, pair_far, far_line, pair_geom, live_blocks):
    blocks, pairs = pair_node.shape[3:]
    blk = positions.shape[1:]
    bx, by, bz = blk
    devices = sizes[0] * sizes[1] * sizes[2]
    outer = blocks // 2
    ndir = len(DIRS)
    rows = 2 * blocks + ndir * outer
    dma = pltpu.SemaphoreType.DMA
    vmem = pl.BlockSpec(memory_space=pltpu.VMEM)
    moved, hist = pl.pallas_call(
        functools.partial(kernel, sizes, blk),
        out_shape=(
            pltpu.VMEM(positions.shape, f32),
            pltpu.VMEM((2, SWEEPS), f32),
        ),
        in_specs=[pl.BlockSpec(memory_space=pltpu.HBM)] * 7,
        out_specs=(vmem, vmem),
        scratch_shapes=[
            pltpu.VMEM(positions.shape, f32),
            pltpu.VMEM((blocks, pairs), i32),
            pltpu.VMEM((blocks, pairs), i32),
            pltpu.VMEM((blocks, 4, pairs), f32),
            pltpu.VMEM((1, blocks), i32),
            pltpu.VMEM((1, blocks), i32),
            pltpu.VMEM((1, 1), i32),
            pltpu.VMEM((ndir, outer, pairs), i32),
            pltpu.VMEM((ndir, 1, blocks), i32),
            pltpu.VMEM((ndir, outer, 4, pairs), f32),
            pltpu.VMEM((3, 3, bx * by, bz), bf16),
            pltpu.VMEM((blocks * pairs, bz), bf16),
            pltpu.VMEM((rows, 2 * blocks), bf16),
            pltpu.VMEM((3, rows, pairs), f32),
            pltpu.VMEM((rows, pairs), i32),
            pltpu.VMEM((rows, pairs), i32),
            pltpu.VMEM((blocks, bz), f32),
            pltpu.VMEM((blocks, pairs), f32),
            pltpu.VMEM((blocks, pairs), f32),
            pltpu.VMEM((blocks, pairs), f32),
            pltpu.VMEM((blocks, 3 * bz), f32),
            pltpu.VMEM((blocks, 3 * bz), f32),
            pltpu.VMEM((8, 128), f32),
            pltpu.VMEM((ndir, 3, outer, pairs), f32),
            pltpu.VMEM((ndir, 3, outer, pairs), f32),
            pltpu.VMEM((SWEEPS - 1, ndir, outer, pairs), f32),
            pltpu.VMEM((SWEEPS - 1, ndir, outer, pairs), f32),
            pltpu.VMEM((SWEEPS, devices, 1, 128), f32),
            dma((7,)),
            dma((2, ndir)),
            dma((3, ndir)),
            dma((ndir,)),
            dma((ndir,)),
            dma((2, ndir)),
            dma,
            dma((2,)),
            pltpu.SemaphoreType.REGULAR,
            pltpu.SemaphoreType.REGULAR,
        ],
        compiler_params=pltpu.CompilerParams(collective_id=0, has_side_effects=True),
    )(live_blocks, pair_node, pair_line, pair_far, far_line, pair_geom, positions)
    return pl.pallas_call(
        finish,
        out_shape=(
            jax.ShapeDtypeStruct(positions.shape, f32),
            jax.ShapeDtypeStruct((2, SWEEPS), f32),
        ),
        in_specs=[vmem, vmem],
        out_specs=(pl.BlockSpec(memory_space=pl.ANY),) * 2,
        scratch_shapes=[dma((2,))],
    )(
        pltpu.with_memory_space_constraint(moved, pltpu.VMEM),
        pltpu.with_memory_space_constraint(hist, pltpu.VMEM),
    )


def solution(mesh):
    sizes = tuple(mesh.shape[a] for a in AXES)
    return jax.shard_map(
        functools.partial(local, sizes),
        mesh=mesh,
        in_specs=(
            P(None, "gx", "gy", "gz"),
            P("gx", "gy", "gz", None, None),
            P("gx", "gy", "gz", None),
            P("gx", "gy", "gz", None, None),
            P("gx", "gy", "gz", None),
            P("gx", "gy", "gz", None, None, None),
            P("gx", "gy", "gz"),
        ),
        out_specs=(P(None, "gx", "gy", "gz"), P()),
        check_vma=False,
    )
```

```python
import functools
import itertools

import jax
import jax.numpy as jnp
from jax import lax
from jax.experimental import pallas as pl
from jax.experimental.pallas import tpu as pltpu
from jax.sharding import PartitionSpec as P

RIM = 3
SWEEPS = 5
RELAX = 0.9
AXES = ("gx", "gy", "gz")
MESH = pl.DeviceIdType.MESH
f32 = jnp.float32
bf16 = jnp.bfloat16
f8 = jnp.float8_e4m3fn
i32 = jnp.int32
DIRS = [(a, s) for a in (1, 0, 2) for s in (1, -1)]


def scope(name):
    return jax.named_scope(name)


def split(x, parts):
    out = []
    for _ in range(parts - 1):
        hi = x.astype(bf16)
        out.append(hi)
        x = x - hi.astype(f32)
    out.append(x.astype(bf16))
    return out


def mm(a, b):
    return lax.dot_general(a, b, (((1,), (0,)), ((), ())), preferred_element_type=f32)


def cat(parts):
    return jnp.concatenate(parts, axis=0)


def take_lanes(x, low, half):
    outs = []
    for h in range(0, low.shape[1], 128):
        idx = low[:, h : h + 128]
        got = jnp.take_along_axis(x[:, :128], idx, axis=1, mode="promise_in_bounds")
        for j in range(1, x.shape[1] // 128):
            more = jnp.take_along_axis(
                x[:, 128 * j : 128 * (j + 1)], idx, axis=1, mode="promise_in_bounds"
            )
            got = jnp.where(half[:, h : h + 128] == j, more, got)
        outs.append(got)
    return jnp.concatenate(outs, axis=1)


def kernel(
    sizes,
    blk,
    live_hbm,
    node_hbm,
    line_hbm,
    far_hbm,
    farline_hbm,
    geom_hbm,
    pos_hbm,
    out_ref,
    hist_ref,
    pos_v,
    node_v,
    far_v,
    geom_v,
    line_v,
    farline_v,
    live_v,
    rfar,
    rline,
    rgeom,
    ppart,
    spare,
    hot,
    amat,
    geo,
    low_ref,
    half_ref,
    cinv,
    gap,
    depth_ref,
    delta,
    wcat,
    acc,
    track,
    vsend,
    vrecv,
    dsend,
    drecv,
    erecv,
    in_sem,
    qs_sem,
    qr_sem,
    vr_sem,
    es_sem,
    er_sem,
    know_sem,
):
    nx, ny, nz = sizes
    bx, by, bz = blk
    devices = nx * ny * nz
    blocks, pairs = gap.shape
    outer = blocks // 2
    lines = bx * by
    base = len(DIRS) * outer
    me = [lax.axis_index(a) for a in AXES]
    mine = (me[0] * ny + me[1]) * nz + me[2]

    def at_offset(off):
        return tuple(lax.rem(me[a] + off[a], sizes[a]) if off[a] else me[a] for a in range(3))

    def neighbour(axis, sign):
        off = [0, 0, 0]
        off[axis] = sign % sizes[axis]
        return at_offset(off)

    def exists(axis, sign):
        return (me[axis] + sign >= 0) & (me[axis] + sign < sizes[axis])

    def along(axis):
        return [tuple(o if a == axis else 0 for a in range(3)) for o in range(1, sizes[axis])]

    def tell(sem, peers):
        for off in peers:
            pl.semaphore_signal(sem, inc=1, device_id=at_offset(off), device_id_type=MESH)

    close = along(2) + along(1) + along(0)

    with scope("entry"):
        barrier = pltpu.get_barrier_semaphore()
        tell(barrier, close)
        loads = [
            pltpu.make_async_copy(src, dst, in_sem.at[i])
            for i, (src, dst) in enumerate(
                [
                    (far_hbm.at[0, 0, 0], far_v),
                    (farline_hbm.at[0, 0], farline_v),
                    (geom_hbm.at[0, 0, 0], geom_v),
                    (pos_hbm, pos_v),
                    (node_hbm.at[0, 0, 0], node_v),
                    (line_hbm.at[0, 0], line_v),
                    (live_hbm.at[0], live_v),
                ]
            )
        ]
        for load in loads:
            load.start()
        loads[0].wait()
        loads[1].wait()
    with scope("barrier"):
        pl.semaphore_wait(barrier, len(close))

    asks = [
        (far_v.at[pl.ds(outer, outer)], rfar),
        (farline_v, rline),
        (geom_v.at[pl.ds(outer, outer)], rgeom),
    ]

    def ask(i, d, axis, sign):
        return pltpu.make_async_remote_copy(
            src_ref=asks[i][0],
            dst_ref=asks[i][1].at[d],
            send_sem=qs_sem.at[i % 2, d],
            recv_sem=qr_sem.at[i, d],
            device_id=neighbour(axis, sign),
            device_id_type=MESH,
        )

    with scope("ask"):
        for d, (axis, sign) in enumerate(DIRS):

            @pl.when(exists(axis, sign))
            def _():
                ask(1, d, axis, sign).start()
                ask(0, d, axis, sign).start()

        tell(know_sem.at[0], along(1))
        loads[2].wait()
        for d, (axis, sign) in enumerate(DIRS):

            @pl.when(exists(axis, sign))
            def _():
                ask(2, d, axis, sign).start()

            @pl.when(jnp.logical_not(exists(axis, -sign)))
            def _():
                rfar[d] = jnp.zeros((outer, pairs), i32)
                rline[d] = jnp.zeros((1, blocks), i32)
                rgeom[d] = jnp.zeros((outer, 4, pairs), f32)

            @pl.when(jnp.logical_not(exists(axis, sign)))
            def _():
                vrecv[d] = jnp.zeros((3, outer, pairs), f32)
                for t in range(SWEEPS - 1):
                    drecv[t, d] = jnp.zeros((outer, pairs), f32)

    with scope("parts"):
        loads[3].wait()
        for c in range(3):
            for i, part in enumerate(split(pos_v[c].reshape(lines, bz), 3)):
                ppart[c, i] = part

    with scope("hot"):
        for load in loads[4:]:
            load.wait()
        lane_node = lax.broadcasted_iota(i32, (pairs, bz), 1).astype(f32)
        node_t = jnp.transpose(node_v[...].astype(f32))
        for b in range(blocks):
            hot[pl.ds(b * pairs, pairs), :] = jnp.where(
                node_t[:, b : b + 1] == lane_node, 1.0, 0.0
            ).astype(f8)

    row_line = line_v[...].astype(f32)
    two = jnp.concatenate([row_line, row_line], axis=1)
    lane_line = lax.broadcasted_iota(i32, (1, lines), 1).astype(f32)

    def column(row, first, n):
        r = lax.broadcasted_iota(i32, (n, blocks), 0)
        l = lax.broadcasted_iota(i32, (n, blocks), 1)
        return jnp.sum(jnp.where(l == r + first, row, 0.0), axis=1, keepdims=True)

    def located(code, shift):
        e = jnp.floor((code + 0.5) / (by + 2 * RIM))
        f = code - e * (by + 2 * RIM)
        e = e - (RIM + shift[0] * bx)
        f = f - (RIM + shift[1] * by)
        inside = (e >= 0) & (e < bx) & (f >= 0) & (f < by)
        return jnp.where(inside, e * by + f, -1.0), inside

    def depth_at(place, inside, shift):
        z = place - (RIM + shift[2] * bz)
        here = inside & (z >= 0) & (z < bz)
        return jnp.where(here, z, 0), jnp.where(here, 1.0, 0.0)

    def halves(node):
        return lax.bitwise_and(node, 127), lax.shift_right_logical(node, 7)

    def values(dst, line):
        own = jnp.where(line == lane_line, 1.0, 0.0).astype(bf16)
        for c in range(3):
            dst[c, 0 : line.shape[0]] = (
                mm(own, ppart[c, 0]) + mm(own, ppart[c, 1]) + mm(own, ppart[c, 2])
            )

    def keep(row, line, low, half):
        n = line.shape[0]
        amat[pl.ds(row, n), :] = jnp.where(line == two, 1.0, 0.0).astype(bf16)
        low_ref[pl.ds(row, n), :] = low
        half_ref[pl.ds(row, n), :] = half

    with scope("known"):
        pl.semaphore_wait(know_sem.at[0], ny - 1)
        tell(know_sem.at[1], along(2))

    def give(c, d, axis, sign):
        return pltpu.make_async_remote_copy(
            src_ref=vsend.at[d, c],
            dst_ref=vrecv.at[d, c],
            send_sem=qs_sem.at[1, d],
            recv_sem=vr_sem.at[d],
            device_id=neighbour(axis, -sign),
            device_id_type=MESH,
        )

    with scope("line_wait"):
        for d, (axis, sign) in enumerate(DIRS):

            @pl.when(exists(axis, sign))
            def _():
                ask(1, d, axis, sign).wait_send()

            @pl.when(exists(axis, -sign))
            def _():
                ask(1, d, axis, sign).wait_recv()

    with scope("lines"):
        shifts = []
        asked_line, asked_in = [], []
        for d, (axis, sign) in enumerate(DIRS):
            shift = [0, 0, 0]
            shift[axis] = sign
            shifts.append(shift)
            line, inside = located(column(rline[d].astype(f32), outer, outer), shift)
            asked_line.append(line)
            asked_in.append(inside)
        asked_line = cat(asked_line)
        values(spare, asked_line)
    with scope("far_wait"):
        for d, (axis, sign) in enumerate(DIRS):

            @pl.when(exists(axis, -sign))
            def _():
                ask(0, d, axis, sign).wait_recv()

    with scope("give"):
        found = [
            depth_at(rfar[d], asked_in[d], shifts[d]) for d in range(len(DIRS))
        ]
        low, half = halves(cat([node for node, _ in found]))
        asked_ok = cat([here for _, here in found])
        for c in range(3):
            got = take_lanes(spare[c], low, half) * asked_ok
            for d in range(len(DIRS)):
                vsend[d, c] = got[d * outer : (d + 1) * outer]
            for d, (axis, sign) in enumerate(DIRS):

                @pl.when(exists(axis, -sign))
                def _():
                    give(c, d, axis, sign).start()

    with scope("keep"):
        keep(0, asked_line, low, half)
    with scope("counts"):
        live = jnp.broadcast_to(live_v[...], (blocks, pairs))
        live_rows = lax.broadcasted_iota(i32, (blocks, pairs), 0) < live

        def expand(stack, step):
            rows = stack.shape[0]
            which = lax.rem(lax.broadcasted_iota(i32, (rows, pairs), 0), step)
            return jnp.concatenate(
                [jnp.where(which == j, stack, 0.0).astype(bf16) for j in range(step)], axis=1
            )

        counts = []
        for g in range(blocks // 8):
            ones = jnp.where(live_rows[8 * g : 8 * g + 8], 1.0, 0.0)
            counts.append(mm(expand(ones, 8), hot[pl.ds(8 * g * pairs, 8 * pairs), :]))
        counts = cat(counts).astype(bf16)
        line_col = column(row_line, 0, blocks)
        same = line_col == row_line
        row_mod = lax.broadcasted_iota(i32, (blocks, blocks), 0)
        col_mod = lax.broadcasted_iota(i32, (blocks, blocks), 1)
        first_col = 1.0 - jnp.max(
            jnp.where(same & (col_mod < row_mod), 1.0, 0.0), axis=1, keepdims=True
        )
        cinv[...] = RELAX / (1.0 + mm(jnp.where(same, 1.0, 0.0).astype(bf16), counts))

    with scope("own"):
        line, inside = located(column(farline_v[...].astype(f32), 0, blocks), (0, 0, 0))
        node, here = depth_at(far_v[...], inside, (0, 0, 0))
        line = cat([line_col, line])
        low, half = halves(cat([node_v[...], node]))
        values(spare, line)
        keep(base, line, low, half)
        start = -geom_v[:, 3, :]
        for c in range(3):
            g = geom_v[:, c, :]
            away = -(g * here)
            geo[c, pl.ds(base, blocks), :] = g
            geo[c, pl.ds(base + blocks, blocks), :] = away
            vals = take_lanes(spare[c, 0 : 2 * blocks], low, half)
            start += g * vals[:blocks] + away * vals[blocks:]
        gap[...] = start
        acc[...] = jnp.zeros_like(acc)
        wcat[...] = jnp.zeros_like(wcat)
        track[...] = jnp.zeros_like(track)

    with scope("geo"):
        for d, (axis, sign) in enumerate(DIRS):

            @pl.when(exists(axis, -sign))
            def _():
                ask(2, d, axis, sign).wait_recv()

        for d in range(len(DIRS)):
            for c in range(3):
                rows = slice(d * outer, (d + 1) * outer)
                geo[c, rows, :] = -(rgeom[d, :, c, :] * asked_ok[rows])

    with scope("give_wait"):
        pl.semaphore_wait(know_sem.at[1], nz - 1)
        for d, (axis, sign) in enumerate(DIRS):

            @pl.when(exists(axis, sign))
            def _():
                pltpu.make_async_copy(vrecv.at[d], vrecv.at[d], vr_sem.at[d]).wait()

        more = jnp.zeros((outer, pairs), f32)
        for c in range(3):
            far = vrecv[0, c]
            for d in range(1, len(DIRS)):
                far = far + vrecv[d, c]
            more = more + geom_v[outer:, c, :] * far
        gap[pl.ds(outer, outer), :] = gap[pl.ds(outer, outer), :] - more

    def answer(t, d, axis, sign):
        return pltpu.make_async_remote_copy(
            src_ref=dsend.at[t, d],
            dst_ref=drecv.at[t, d],
            send_sem=qs_sem.at[1, d],
            recv_sem=qr_sem.at[lax.rem(t, 2), d],
            device_id=neighbour(axis, -sign),
            device_id_type=MESH,
        )

    def hops(off):
        x, core = off[2] // 2, off[2] % 2
        far = [min(o, s - o) for o, s in ((off[0], nx), (off[1], ny), (x, nz // 2))]
        return sum(far) + 0.3 * core

    everyone = sorted(
        (o for o in itertools.product(range(nx), range(ny), range(nz)) if any(o)),
        key=hops,
        reverse=True,
    )

    def to_all(t):
        ref = erecv.at[t, mine]
        for off in everyone:
            pltpu.make_async_remote_copy(
                src_ref=ref,
                dst_ref=ref,
                send_sem=es_sem,
                recv_sem=er_sem.at[lax.rem(t, 2)],
                device_id=at_offset(off),
                device_id_type=MESH,
            ).start()

    def from_all(t):
        others = erecv.at[t, pl.ds(0, devices - 1)]
        pltpu.make_async_copy(others, others, er_sem.at[lax.rem(t, 2)]).wait()
        rows = [erecv[t, i] for i in range(devices)]
        while len(rows) > 1:
            rows = [a + b for a, b in zip(rows[::2], rows[1::2])] + rows[len(rows) & ~1 :]
        return rows[0]

    def lanes_sum(x):
        x = jnp.sum(x, axis=0, keepdims=True)
        out = x[:, :128]
        for j in range(1, x.shape[1] // 128):
            out = out + x[:, 128 * j : 128 * (j + 1)]
        return out

    lane = lax.broadcasted_iota(i32, (1, 128), 1)

    def dots(row, n, moved):
        low = low_ref[row : row + n, :]
        half = half_ref[row : row + n, :]
        total = geo[0, row : row + n] * take_lanes(moved[:, :bz], low, half)
        for c in range(1, 3):
            total += geo[c, row : row + n] * take_lanes(
                moved[:, c * bz : (c + 1) * bz], low, half
            )
        return total

    def depths():
        depth = jnp.where(live_rows, jnp.maximum(-gap[...], 0.0), 0.0)
        depth_ref[...] = depth
        return lanes_sum(depth * depth)

    def scatter():
        for g in range(blocks // 8):
            lo, hi = 8 * g, 8 * g + 8
            depth = depth_ref[lo:hi, :]
            terms = cat([depth * geo[c, base + lo : base + hi] for c in range(3)])
            top = terms.astype(bf16).astype(f32)
            sums = mm(expand(cat([top, terms - top]), 8), hot[pl.ds(lo * pairs, 8 * pairs), :])
            sums = sums[:24] + sums[24:]
            for c in range(3):
                wcat[lo:hi, c * bz : (c + 1) * bz] = sums[8 * c : 8 * c + 8] * cinv[lo:hi, :]
        return cat(split(wcat[...], 2))

    def residual(near):
        return jnp.sum(lanes_sum(near * near * first_col), axis=1, keepdims=True)

    def note(t, energy, scale):
        track[0:1, :] = jnp.where(lane == t, energy, track[0:1, :])
        track[1:2, :] = jnp.where(lane == t, scale, track[1:2, :])
        acc[...] = acc[...] + scale * wcat[...]

    def ratio(energy):
        return 1.0 / (1.0 + energy / (blocks * pairs * devices))

    def sweep(t, energy, last):
        with scope("note"):
            note(t - 1, energy, ratio(energy))
        with scope("scatter"):
            parts = scatter()
        with scope("respond"):
            total = dots(0, base, mm(amat[0:base, :], parts))
            for d in range(len(DIRS)):
                dsend[t, d] = total[d * outer : (d + 1) * outer]
            for d, (axis, sign) in enumerate(DIRS):

                @pl.when(exists(axis, -sign))
                def _():
                    answer(t, d, axis, sign).start()

        with scope("step"):
            moved = mm(amat[base : base + 2 * blocks, :], parts)
            resid = residual(moved[:blocks])
            track[2:3, :] = jnp.where(lane == t, resid, track[2:3, :])
            step = dots(base, 2 * blocks, moved)
            delta[...] = step[:blocks] + step[blocks:]
        with scope("answer_wait"):
            for d, (axis, sign) in enumerate(DIRS):

                @pl.when(exists(axis, sign))
                def _():
                    answer(t, d, axis, sign).wait_recv()

            more = drecv[t, 0]
            for d in range(1, len(DIRS)):
                more = more + drecv[t, d]
            delta[pl.ds(outer, outer), :] = delta[pl.ds(outer, outer), :] + more
        with scope("energy_wait"):
            energy = jnp.sum(from_all(t), axis=1, keepdims=True)
        with scope("energy"):
            gap[...] = gap[...] + ratio(energy) * delta[...]
            squares = depths()
            if last:
                return energy, squares
            erecv[t + 1, mine] = squares
            to_all(t + 1)
        return energy

    with scope("energy"):
        erecv[0, mine] = depths()
        to_all(0)

    zero = jnp.zeros((1, 1), f32)
    energy = lax.fori_loop(0, SWEEPS - 2, lambda t, energy: sweep(t, energy, False), zero)
    energy, squares = sweep(SWEEPS - 2, energy, True)
    end = SWEEPS - 1
    with scope("scatter"):
        note(end - 1, energy, ratio(energy))
        parts = scatter()
    with scope("resid"):
        resid = residual(mm(amat[base : base + blocks, :], parts))
        energy = jnp.sum(squares, axis=1, keepdims=True)
        row = jnp.where(lane == end, resid, track[2:3, :])
        erecv[end, mine] = jnp.where(lane == SWEEPS, energy, row)
        to_all(end)
    with scope("join"):
        row = lax.broadcasted_iota(i32, (lines, 2 * blocks), 0).astype(f32)
        spread = jnp.where(row == two, 1.0, 0.0).astype(bf16)
        before = mm(spread, cat(split(acc[...], 2)))
        ahead = mm(spread, parts)
        for c in range(3):
            pos_v[c] = pos_v[c] + before[:, c * bz : (c + 1) * bz].reshape(bx, by, bz)
            out_ref[c] = ahead[:, c * bz : (c + 1) * bz].reshape(bx, by, bz)
        for d, (axis, sign) in enumerate(DIRS):

            @pl.when(exists(axis, sign))
            def _():
                sent = geo.at[0, pl.ds(0, 5 * outer)]
                pltpu.make_async_copy(sent, sent, qs_sem.at[0, d]).wait()

            @pl.when(exists(axis, -sign))
            def _():
                sent = geo.at[0, pl.ds(0, (SWEEPS + 2) * outer)]
                pltpu.make_async_copy(sent, sent, qs_sem.at[1, d]).wait()

    with scope("last_wait"):
        sums = from_all(end)
    with scope("end"):
        energy = sums[:, SWEEPS : SWEEPS + 1]
        scale = ratio(energy)
        for c in range(3):
            out_ref[c] = pos_v[c] + jnp.broadcast_to(scale[:, None], (1, 1, 1)) * out_ref[c]
        n = hist_ref.shape[1]
        energies = jnp.where(lane == end, energy, track[0:1, :])
        scales = jnp.where(lane == end, scale, track[1:2, :])
        hist_ref[0:1, :] = jnp.sqrt(1.0 + energies / (blocks * pairs))[:, :n]
        hist_ref[1:2, :] = jnp.sqrt(1.0 + scales * scales * sums / (bx * by * bz))[:, :n]
        sent = erecv.at[pl.ds(0, SWEEPS), pl.ds(0, devices - 1)]
        pltpu.make_async_copy(sent, sent, es_sem).wait()


def finish(moved, hist, out_hbm, hist_hbm, sem):
    copies = [
        pltpu.make_async_copy(moved, out_hbm, sem.at[0]),
        pltpu.make_async_copy(hist, hist_hbm, sem.at[1]),
    ]
    for copy in copies:
        copy.start()
    for copy in copies:
        copy.wait()


def local(sizes, positions, pair_node, pair_line, pair_far, far_line, pair_geom, live_blocks):
    blocks, pairs = pair_node.shape[3:]
    blk = positions.shape[1:]
    bx, by, bz = blk
    devices = sizes[0] * sizes[1] * sizes[2]
    outer = blocks // 2
    ndir = len(DIRS)
    rows = 2 * blocks + ndir * outer
    dma = pltpu.SemaphoreType.DMA
    vmem = pl.BlockSpec(memory_space=pltpu.VMEM)
    moved, hist = pl.pallas_call(
        functools.partial(kernel, sizes, blk),
        out_shape=(
            pltpu.VMEM(positions.shape, f32),
            pltpu.VMEM((2, SWEEPS), f32),
        ),
        in_specs=[pl.BlockSpec(memory_space=pltpu.HBM)] * 7,
        out_specs=(vmem, vmem),
        scratch_shapes=[
            pltpu.VMEM(positions.shape, f32),
            pltpu.VMEM((blocks, pairs), i32),
            pltpu.VMEM((blocks, pairs), i32),
            pltpu.VMEM((blocks, 4, pairs), f32),
            pltpu.VMEM((1, blocks), i32),
            pltpu.VMEM((1, blocks), i32),
            pltpu.VMEM((1, 1), i32),
            pltpu.VMEM((ndir, outer, pairs), i32),
            pltpu.VMEM((ndir, 1, blocks), i32),
            pltpu.VMEM((ndir, outer, 4, pairs), f32),
            pltpu.VMEM((3, 3, bx * by, bz), bf16),
            pltpu.VMEM((3, ndir * outer, bz), f32),
            pltpu.VMEM((blocks * pairs, bz), f8),
            pltpu.VMEM((rows, 2 * blocks), bf16),
            pltpu.VMEM((3, rows, pairs), f32),
            pltpu.VMEM((rows, pairs), i32),
            pltpu.VMEM((rows, pairs), i32),
            pltpu.VMEM((blocks, bz), f32),
            pltpu.VMEM((blocks, pairs), f32),
            pltpu.VMEM((blocks, pairs), f32),
            pltpu.VMEM((blocks, pairs), f32),
            pltpu.VMEM((blocks, 3 * bz), f32),
            pltpu.VMEM((blocks, 3 * bz), f32),
            pltpu.VMEM((8, 128), f32),
            pltpu.VMEM((ndir, 3, outer, pairs), f32),
            pltpu.VMEM((ndir, 3, outer, pairs), f32),
            pltpu.VMEM((SWEEPS - 1, ndir, outer, pairs), f32),
            pltpu.VMEM((SWEEPS - 1, ndir, outer, pairs), f32),
            pltpu.VMEM((SWEEPS, devices, 1, 128), f32),
            dma((7,)),
            dma((2, ndir)),
            dma((3, ndir)),
            dma((ndir,)),
            dma,
            dma((2,)),
            pltpu.SemaphoreType.REGULAR((2,)),
        ],
        compiler_params=pltpu.CompilerParams(collective_id=0, has_side_effects=True),
    )(live_blocks, pair_node, pair_line, pair_far, far_line, pair_geom, positions)
    return pl.pallas_call(
        finish,
        out_shape=(
            jax.ShapeDtypeStruct(positions.shape, f32),
            jax.ShapeDtypeStruct((2, SWEEPS), f32),
        ),
        in_specs=[vmem, vmem],
        out_specs=(pl.BlockSpec(memory_space=pl.ANY),) * 2,
        scratch_shapes=[dma((2,))],
    )(
        pltpu.with_memory_space_constraint(moved, pltpu.VMEM),
        pltpu.with_memory_space_constraint(hist, pltpu.VMEM),
    )


def solution(mesh):
    sizes = tuple(mesh.shape[a] for a in AXES)
    return jax.shard_map(
        functools.partial(local, sizes),
        mesh=mesh,
        in_specs=(
            P(None, "gx", "gy", "gz"),
            P("gx", "gy", "gz", None, None),
            P("gx", "gy", "gz", None),
            P("gx", "gy", "gz", None, None),
            P("gx", "gy", "gz", None),
            P("gx", "gy", "gz", None, None, None),
            P("gx", "gy", "gz"),
        ),
        out_specs=(P(None, "gx", "gy", "gz"), P()),
        check_vma=False,
    )
```
